64 devices in a mesh: dp: 4 (over x, y), fsdp: 16 (over z, core).
Axes of the slice: x: 2, y: 2, z: 8, core: 2. Of those that a mesh axis runs over, the one named last changes fastest.
The devices are a block of a 4x4x8 slice.
Arguments:
- images: bfloat16 [192, 256, 1536], P(('dp', 'fsdp')), parts along dimension 0
- ln1_scale: bfloat16 [2, 1536], P(None, 'fsdp')
- ln1_bias: bfloat16 [2, 1536], P(None, 'fsdp')
- w_qkv: bfloat16 [2, 1536, 3, 16, 96], P(None, 'fsdp')
- b_qkv: bfloat16 [2, 4608], P(None, 'fsdp')
- w_out: bfloat16 [2, 1536, 1536], P(None, 'fsdp')
- b_out: bfloat16 [2, 1536], P(None, 'fsdp')
- ln2_scale: bfloat16 [2, 1536], P(None, 'fsdp')
- ln2_bias: bfloat16 [2, 1536], P(None, 'fsdp')
- w_up: bfloat16 [2, 1536, 6144], P(None, 'fsdp')
- b_up: bfloat16 [2, 6144], P(None, 'fsdp')
- w_down: bfloat16 [2, 6144, 1536], P(None, 'fsdp')
- b_down: bfloat16 [2, 1536], P(None, 'fsdp')
Outputs:
- output: bfloat16 [192, 256, 1536], P(('dp', 'fsdp')), parts along dimension 0
There are 4 independent parts. The reference program is written for one: setup_inputs(seed, part) draws one part's arguments, and reference() takes and returns one part's arrays. A program takes and returns all parts, laid end to end along the dimension named above; an argument that names none is the same for every part.
All inputs are finite; a program needn't handle non-finite values.
Results may differ from the reference program's by a relative error of at most 0.010846.
Values are sent between devices in bfloat16 or wider.
A program may use at most 768 MiB of HBM per device.

```python
import jax
import jax.numpy as jnp
from jax import lax

BATCH = 48
TOKENS = 256
MODEL_DIM = 1536
NUM_HEADS = 16
HEAD_DIM = 96
MLP_DIM = 6144
MLP_PAD = 6144
LAYERS = 2
LN_EPS = 1e-6


def setup_inputs(seed: int = 0, part: int = 0) -> dict:
    keys = jax.random.split(jax.random.key(seed), 13)
    width_scale = MODEL_DIM ** -0.5
    keep_cols = (jnp.arange(MLP_PAD) < MLP_DIM).astype(jnp.float32)
    vec_shape = (LAYERS, MODEL_DIM)

    def normal(key_index, dims):
        return jax.random.normal(keys[key_index], dims, jnp.float32)

    tokens = jax.random.normal(jax.random.fold_in(keys[0], part), (BATCH, TOKENS, MODEL_DIM), jnp.float32)
    arrays = {
        'images': tokens,
        'ln1_scale': 1.0 + 0.4 * normal(1, vec_shape),
        'ln1_bias': 0.4 * normal(2, vec_shape),
        'w_qkv': normal(3, (LAYERS, MODEL_DIM, 3, NUM_HEADS, HEAD_DIM)) * width_scale,
        'b_qkv': 0.5 * normal(4, (LAYERS, 3 * MODEL_DIM)),
        'w_out': normal(5, (LAYERS, MODEL_DIM, MODEL_DIM)) * width_scale,
        'b_out': 0.4 * normal(6, vec_shape),
        'ln2_scale': 1.0 + 0.4 * normal(7, vec_shape),
        'ln2_bias': 0.4 * normal(8, vec_shape),
        'w_up': normal(9, (LAYERS, MODEL_DIM, MLP_PAD)) * width_scale * keep_cols,
        'b_up': 0.5 * normal(10, (LAYERS, MLP_PAD)) * keep_cols,
        'w_down': normal(11, (LAYERS, MLP_PAD, MODEL_DIM)) * (MLP_DIM ** -0.5) * keep_cols[:, None],
        'b_down': 0.4 * normal(12, vec_shape),
    }
    return {name: value.astype(jnp.bfloat16) for name, value in arrays.items()}


def layer_norm(values, ln_scale, ln_shift):
    centered = values.astype(jnp.float32)
    centered = centered - jnp.mean(centered, axis=-1, keepdims=True)
    variance = jnp.mean(jnp.square(centered), axis=-1, keepdims=True)
    normed = centered * lax.rsqrt(variance + LN_EPS)
    return (normed * ln_scale.astype(jnp.float32) + ln_shift.astype(jnp.float32)).astype(jnp.bfloat16)


def encoder_layer(tokens, params):
    (ln1_scale, ln1_bias, w_qkv, b_qkv, w_out, b_out, ln2_scale, ln2_bias, w_up, b_up, w_down, b_down) = params
    normed = layer_norm(tokens, ln1_scale, ln1_bias)
    qkv_flat = jnp.dot(normed, w_qkv.reshape(MODEL_DIM, 3 * MODEL_DIM), preferred_element_type=jnp.float32)
    qkv_heads = (qkv_flat + b_qkv.astype(jnp.float32)).astype(jnp.bfloat16).reshape(TOKENS, 3, NUM_HEADS, HEAD_DIM)
    queries = qkv_heads[:, 0].astype(jnp.float32)
    key_heads = qkv_heads[:, 1].astype(jnp.float32)
    values = qkv_heads[:, 2].astype(jnp.float32)
    scores = jnp.einsum('qhe,khe->hqk', queries, key_heads) * (HEAD_DIM ** -0.5)
    attn_probs = jax.nn.softmax(scores, axis=-1).astype(jnp.bfloat16).astype(jnp.float32)
    attended = jnp.einsum('hqk,khe->qhe', attn_probs, values).astype(jnp.bfloat16).reshape(TOKENS, MODEL_DIM)
    projected = jnp.dot(attended, w_out, preferred_element_type=jnp.float32) + b_out.astype(jnp.float32)
    after_attn = (tokens.astype(jnp.float32) + projected).astype(jnp.bfloat16)
    normed_mlp = layer_norm(after_attn, ln2_scale, ln2_bias)
    hidden = jnp.dot(normed_mlp, w_up[:, :MLP_DIM], preferred_element_type=jnp.float32) + b_up[:MLP_DIM].astype(jnp.float32)
    gelu_out = jax.nn.gelu(hidden, approximate=True).astype(jnp.bfloat16)
    down_proj = jnp.dot(gelu_out, w_down[:MLP_DIM], preferred_element_type=jnp.float32) + b_down.astype(jnp.float32)
    return (after_attn.astype(jnp.float32) + down_proj).astype(jnp.bfloat16), None


def reference(images, ln1_scale, ln1_bias, w_qkv, b_qkv, w_out, b_out, ln2_scale, ln2_bias, w_up, b_up, w_down, b_down):
    params = (ln1_scale, ln1_bias, w_qkv, b_qkv, w_out, b_out, ln2_scale, ln2_bias, w_up, b_up, w_down, b_down)

    def one_image(tokens):
        encoded, _ = lax.scan(encoder_layer, tokens, params)
        return encoded

    return lax.map(one_image, images)
```

```python
import functools
import math

import jax
import jax.numpy as jnp
from jax import lax
from jax.experimental import pallas as pl
from jax.experimental.pallas import tpu as pltpu
from jax.sharding import PartitionSpec as P

LN_EPS = 1e-6
MESH = pl.DeviceIdType.MESH
CORES = 2
SUB = 3
COMPUTE = True

LN1_S, LN1_B, B_QKV, B_OUT, LN2_S, LN2_B, B_UP, B_DOWN = range(8)
QKV, OUT, UP, DOWN = range(4)
GROUPS = (((0, QKV),), ((0, OUT), (0, UP)), ((0, DOWN),), ((1, QKV), (1, OUT)), ((1, UP),), ((1, DOWN),))
F32 = jnp.float32
BF16 = jnp.bfloat16


def _kernel(dims, x_in, vec_in, *refs):
    ny, nz, heads, hd = dims
    win, refs = refs[:4], refs[4:]
    out_ref, refs = refs[0], refs[1:]
    gath, refs = refs[:4], refs[4:]
    x, h, qkv, g, acc, wt = refs[:6]
    bounce, refs = refs[6:10], refs[10:]
    vecg, vrow = refs[:2]
    (rec_a, rec_b, rec_x, rec_y, rec_d, rec_l, snd_a, snd_b, snd_x, snd_y, snd_d, snd_v, vec_a, vec_b, vec_d, loc, tile_sem,
     out_sem) = refs[2:]

    rows, width = x.shape
    mblocks = 3
    mrows = rows // mblocks
    steps = nz - 1
    ticks = steps * SUB

    d = lax.axis_index('dp')
    f = lax.axis_index('fsdp')
    z, c = f // CORES, f % CORES
    up_dev = (d, ((z + 1) % nz) * CORES + c)
    dn_dev = (d, ((z + nz - 1) % nz) * CORES + c)
    sib_dev = (d, z * CORES + (CORES - 1 - c))
    x_dev = (d + ny * (1 - 2 * ((d // ny) % 2)), f)
    y_dev = (d + 1 - 2 * (d % 2), f)
    par = (d // ny + d % ny) % 2
    qa, qb = 2 * par, 2 * par + 1
    qx, qy = 2 * (1 - par), 2 * (1 - par) + 1

    barrier = pltpu.get_barrier_semaphore()
    for dev in (up_dev, dn_dev, sib_dev, x_dev, y_dev):
        pl.semaphore_signal(barrier, inc=1, device_id=dev, device_id_type=MESH)
    pl.semaphore_wait(barrier, 5)

    def remote(src, dst, ssem, rsem, dev):
        return pltpu.make_async_remote_copy(src_ref=src, dst_ref=dst, send_sem=ssem, recv_sem=rsem, device_id=dev,
                                            device_id_type=MESH)

    def wid(w):
        return w[0] * 4 + w[1]

    def shard_rows(kind):
        return win[kind].shape[1]

    def part(ref, w, origin, q, j):
        l, kind = w
        r = shard_rows(kind)
        if kind == DOWN:
            n = r // SUB
            cols = ref.shape[2] // 4
            return ref.at[l, pl.ds(pl.multiple_of(origin * r + j * n, 8), n), pl.ds(pl.multiple_of(q * cols, 128), cols)]
        n = r // (4 * SUB)
        return ref.at[l, pl.ds(pl.multiple_of(origin * r + q * (r // 4) + j * n, 8), n), :]

    def amount(w, quarters):
        l, kind = w
        r, cols = shard_rows(kind), gath[kind].shape[2]
        if kind == DOWN and quarters % 4:
            return gath[kind].at[l, pl.ds(0, quarters * r), pl.ds(0, cols // 4)]
        return gath[kind].at[l, pl.ds(0, quarters * (r // 4)), :]

    def wait_bytes(view, sem):
        pltpu.make_async_copy(view, view, sem).wait()

    def d2d_sem(w, t):
        return rec_l.at[t] if w == GROUPS[-1][-1] else rec_d.at[wid(w)]

    def own_send(grp, j):
        for w in GROUPS[grp]:
            l, kind = w
            remote(part(win[kind], w, 0, qa, j), part(gath[kind], w, f, qa, j), snd_a.at[wid(w)], rec_a.at[wid(w), 0, j], up_dev).start()
            remote(part(win[kind], w, 0, qb, j), part(gath[kind], w, f, qb, j), snd_b.at[wid(w)], rec_b.at[wid(w), 0, j], dn_dev).start()

    def own_d2d(grp):
        for w in GROUPS[grp]:
            l, kind = w
            r = shard_rows(kind)
            remote(win[kind].at[l], gath[kind].at[l, pl.ds(pl.multiple_of(f * r, 8), r), :], snd_d.at[wid(w)], d2d_sem(w, 0), sib_dev).start()

    def xy_arrive(grp, t, j):
        oa = ((z - t + nz) % nz) * CORES + c
        ob = ((z + t) % nz) * CORES + c
        for w in GROUPS[grp]:
            l, kind = w
            px, py = part(gath[kind], w, oa, qx, j), part(gath[kind], w, ob, qy, j)
            remote(px, px, snd_x.at[wid(w)], rec_x.at[wid(w), t - 1, j], x_dev).wait_recv()
            remote(px, px, snd_d.at[wid(w)], d2d_sem(w, t), sib_dev).start()
            remote(py, py, snd_y.at[wid(w)], rec_y.at[wid(w), t - 1, j], y_dev).wait_recv()
            remote(py, py, snd_d.at[wid(w)], d2d_sem(w, t), sib_dev).start()

    def tick(grp, i, early):
        t, j = i // SUB + 1, i % SUB
        oa = ((z - t + nz) % nz) * CORES + c
        ob = ((z + t) % nz) * CORES + c
        for w in GROUPS[grp]:
            l, kind = w
            for o, q, snd, rec, dev in ((oa, qa, snd_a, rec_a, up_dev), (ob, qb, snd_b, rec_b, dn_dev)):
                p = part(gath[kind], w, o, q, j)
                remote(p, p, snd.at[wid(w)], rec.at[wid(w), t - 1, j], dev).wait_recv()

                @pl.when(t < steps)
                def _():
                    remote(p, p, snd.at[wid(w)], rec.at[wid(w), t, j], dev).start()

            pa, pb = part(gath[kind], w, oa, qa, j), part(gath[kind], w, ob, qb, j)
            remote(pa, pa, snd_x.at[wid(w)], rec_x.at[wid(w), t - 1, j], x_dev).start()
            remote(pb, pb, snd_y.at[wid(w)], rec_y.at[wid(w), t - 1, j], y_dev).start()
            remote(pa, pa, snd_d.at[wid(w)], d2d_sem(w, t), sib_dev).start()
            remote(pb, pb, snd_d.at[wid(w)], d2d_sem(w, t), sib_dev).start()
        if grp + 1 < len(GROUPS):

            @pl.when(t == steps - 1)
            def _():
                own_send(grp + 1, j)

        if grp == 0:
            half = nz // 2
            va, vb = vecg.at[oa], vecg.at[ob]

            @pl.when(jnp.logical_and(j == 0, t <= half))
            def _():
                remote(va, va, snd_v.at[0], vec_a.at[t - 1], up_dev).wait_recv()

                @pl.when(t < half)
                def _():
                    remote(va, va, snd_v.at[0], vec_a.at[t], up_dev).start()

                remote(va, va, snd_v.at[2], vec_d, sib_dev).start()

            @pl.when(jnp.logical_and(j == 0, t < half))
            def _():
                remote(vb, vb, snd_v.at[1], vec_b.at[t - 1], dn_dev).wait_recv()

                @pl.when(t < half - 1)
                def _():
                    remote(vb, vb, snd_v.at[1], vec_b.at[t], dn_dev).start()

                remote(vb, vb, snd_v.at[2], vec_d, sib_dev).start()

        if not early:
            xy_arrive(grp, t - 1, j)
        elif grp > 0:
            xy_arrive(grp - 1, steps, j)

    def run(grp, lo, hi, total=0, unit=None):
        def body(i, carry):
            tick(grp, i, hi <= SUB)
            if unit is not None and COMPUTE:
                k = i - lo
                lax.fori_loop((k * total) // (hi - lo), ((k + 1) * total) // (hi - lo), lambda u, cc: (unit(u), cc)[1], 0)
            return carry

        lax.fori_loop(lo, hi, body, 0)

    def await_group(grp):
        for w in GROUPS[grp]:
            wait_bytes(amount(w, 4 * nz), rec_d.at[wid(w)])

    def vec(l, k, n, width_):
        return vrow[pl.ds(l * 8 + k, 1), pl.ds(n, width_)]

    def ln_unit(l, ks, kb):
        n = 64

        def unit(u):
            sl = pl.ds(pl.multiple_of(u * n, n), n)
            v = x[sl, :].astype(F32)
            v = v - jnp.mean(v, axis=-1, keepdims=True)
            var = jnp.mean(v * v, axis=-1, keepdims=True)
            y = v * lax.rsqrt(var + LN_EPS)
            h[sl, :] = (y * vec(l, ks, 0, width) + vec(l, kb, 0, width)).astype(BF16)

        return rows // n, unit

    kt, nt = wt.shape[1], wt.shape[2]

    def tile_copy(w, i, kparts):
        l, kind = w
        n, k = i // kparts, i % kparts
        src = gath[kind].at[l, pl.ds(pl.multiple_of(k * kt, 8), kt), pl.ds(pl.multiple_of(n * nt, 128), nt)]
        return pltpu.make_async_copy(src, wt.at[i % 2], tile_sem.at[i % 2])

    def mm_unit(w, a_ref, epilogue):
        l, kind = w
        kparts = (gath[kind].shape[1]) // kt
        ntiles = gath[kind].shape[2] // nt * kparts

        def unit(u):
            i, mb = u // mblocks, u % mblocks
            n, k = i // kparts, i % kparts

            @pl.when(mb == 0)
            def _():
                tile_copy(w, i, kparts).wait()

                @pl.when(i + 1 < ntiles)
                def _():
                    tile_copy(w, i + 1, kparts).start()

            msl = pl.ds(pl.multiple_of(mb * mrows, mrows), mrows)
            nsl = pl.ds(pl.multiple_of(n * nt, 128), nt)
            ksl = pl.ds(pl.multiple_of(k * kt, 128), kt) if kparts > 1 else slice(None)
            res = jnp.dot(a_ref[msl, ksl], wt[i % 2], preferred_element_type=F32)
            epilogue(res, msl, nsl, n * nt, k)

        return ntiles * mblocks, unit, functools.partial(lambda: tile_copy(w, 0, kparts).start())

    def lanes(n):
        return pl.multiple_of(n, 128)

    def qkv_epi(l):
        def epi(res, msl, nsl, n0, k):
            qkv[msl, nsl] = (res + vec(l, B_QKV, lanes(n0), nt)).astype(BF16)

        return epi

    def out_epi(l):
        def epi(res, msl, nsl, n0, k):
            x[msl, nsl] = (x[msl, nsl].astype(F32) + (res + vec(l, B_OUT, lanes(n0), nt))).astype(BF16)

        return epi

    def up_epi(l):
        def epi(res, msl, nsl, n0, k):
            g[msl, nsl] = jax.nn.gelu(res + vec(l, B_UP, lanes(n0), nt), approximate=True).astype(BF16)

        return epi

    def down_epi(l, kparts):
        def epi(res, msl, nsl, n0, k):
            @pl.when(k == 0)
            def _():
                acc[msl, nsl] = res

            @pl.when(jnp.logical_and(k > 0, k < kparts - 1))
            def _():
                acc[msl, nsl] += res

            @pl.when(k == kparts - 1)
            def _():
                x[msl, nsl] = (x[msl, nsl].astype(F32) + (acc[msl, nsl] + res + vec(l, B_DOWN, lanes(n0), nt))).astype(BF16)

        return epi

    seq = 2 * 128
    hg = 4

    def attn_unit():
        lane = lax.broadcasted_iota(jnp.int32, (1, seq), 1)
        gw = hg * hd
        scale = hd ** -0.5

        def window(q2, k2, v2, offs):
            ms = [jnp.logical_and(lane >= o, lane < o + hd).astype(BF16) for o in offs]
            ks = jnp.concatenate([k2 * m for m in ms], axis=0)
            vs = jnp.concatenate([v2 * m for m in ms], axis=0)
            s = lax.dot_general(q2, ks, (((1,), (1,)), ((), ())), preferred_element_type=F32) * scale
            ps = []
            for i in range(len(offs)):
                si = s[:, i * seq:(i + 1) * seq]
                e = jnp.exp(si - jnp.max(si, axis=-1, keepdims=True))
                ps.append((e / jnp.sum(e, axis=-1, keepdims=True)).astype(BF16))
            return jnp.dot(jnp.concatenate(ps, axis=1), vs, preferred_element_type=F32)

        def unit(u):
            img, grp = u // (heads // hg), u % (heads // hg)
            msl = pl.ds(pl.multiple_of(img * seq, seq), seq)

            def win_(base, off):
                return qkv[msl, pl.ds(pl.multiple_of(base * width + grp * gw + off, 128), seq)]

            o0 = window(win_(0, 0), win_(1, 0), win_(2, 0), (0, hd))
            o1 = window(win_(0, 128), win_(1, 128), win_(2, 128), (2 * hd - 128, 3 * hd - 128))
            c0 = grp * gw
            h[msl, pl.ds(pl.multiple_of(c0, 128), 128)] = o0[:, :128].astype(BF16)
            h[msl, pl.ds(pl.multiple_of(c0 + 128, 128), 128)] = (o0[:, 128:] + o1[:, :128]).astype(BF16)
            h[msl, pl.ds(pl.multiple_of(c0 + 256, 128), 128)] = o1[:, 128:].astype(BF16)

        return (rows // seq) * (heads // hg), unit

    def build_vectors():
        wait_bytes(vecg.at[pl.ds(0, nz)], vec_d)
        nd = nz * CORES
        for a in range(nd // 4):
            s = vecg[4 * a].astype(F32)
            for r in range(1, 4):
                s = s + vecg[4 * a + r].astype(F32)
            for l in range(2):
                for k in (LN1_S, LN1_B, B_OUT, LN2_S, LN2_B, B_DOWN):
                    wv = width // (nd // 4)
                    vrow[l * 8 + k:l * 8 + k + 1, a * wv:(a + 1) * wv] = s[l * 8 + k:l * 8 + k + 1, :wv]
                wv = 3 * width // (nd // 4)
                vrow[l * 8 + B_QKV:l * 8 + B_QKV + 1, a * wv:(a + 1) * wv] = s[l * 8 + B_QKV:l * 8 + B_QKV + 1, :wv]
        wv = vrow.shape[1] // nd
        for o in range(nd):
            s = vecg[o].astype(F32)
            for l in range(2):
                vrow[l * 8 + B_UP:l * 8 + B_UP + 1, o * wv:(o + 1) * wv] = s[l * 8 + B_UP:l * 8 + B_UP + 1, :wv]

    last = GROUPS[-1][-1]
    zrows = CORES * win[DOWN].shape[1]
    dq = width // 4

    def slot_copies(t):
        za, zb = (z - t + nz) % nz, (z + t) % nz
        for n, (zz, q, r0, c0) in enumerate(((za, 0, 0, 0), (za, 2, 0, dq), (zb, 1, zrows, 0), (zb, 3, zrows, dq))):
            yield pltpu.make_async_copy(
                gath[DOWN].at[last[0], pl.ds(pl.multiple_of(zz * zrows, 8), zrows), pl.ds(q * dq, dq)],
                wt.at[t % 2, pl.ds(r0, zrows), pl.ds(c0, dq)], tile_sem.at[t % 2])

    def slot_ready(t):
        l, kind = last
        wait_bytes(gath[kind].at[l, pl.ds(0, win[kind].shape[1]), :], rec_l.at[t])
        for cp in slot_copies(t):
            cp.start()

    def slot_wait(t):
        pltpu.make_async_copy(wt.at[t % 2], wt.at[t % 2], tile_sem.at[t % 2]).wait()

    def slot_compute(t):
        za, zb = (z - t + nz) % nz, (z + t) % nz

        def body(mb, carry):
            msl = pl.ds(pl.multiple_of(mb * mrows, mrows), mrows)
            for zz, r0, cols in ((za, 0, (0, 2)), (zb, zrows, (1, 3))):
                res = jnp.dot(g[msl, pl.ds(pl.multiple_of(zz * zrows, 128), zrows)], wt[t % 2, r0:r0 + zrows, :], preferred_element_type=F32)
                for n, q in enumerate(cols):
                    acc[msl, q * dq:(q + 1) * dq] += res[:, n * dq:(n + 1) * dq]
            return carry

        lax.fori_loop(0, mblocks, body, 0)

    vec_mine = vecg.at[f]
    remote(vec_in, vec_mine, snd_v.at[0], vec_a.at[0], up_dev).start()
    remote(vec_in, vec_mine, snd_v.at[1], vec_b.at[0], dn_dev).start()
    remote(vec_in, vec_mine, snd_v.at[2], vec_d, sib_dev).start()
    for j in range(SUB):
        own_send(0, j)
    own_d2d(0)
    load_x = pltpu.make_async_copy(x_in, x, out_sem.at[0])
    load_x.start()
    load_v = pltpu.make_async_copy(vec_in, vec_mine, out_sem.at[1])
    load_v.start()
    for l in range(2):
        for kind in range(4):
            pltpu.make_async_copy(win[kind].at[l], bounce[kind], loc.at[kind]).start()
        for kind in range(4):
            r = shard_rows(kind)
            pltpu.make_async_copy(win[kind].at[l], bounce[kind], loc.at[kind]).wait()
            pltpu.make_async_copy(bounce[kind], gath[kind].at[l, pl.ds(pl.multiple_of(f * r, 8), r), :], loc.at[kind]).start()
        for kind in range(4):
            r = shard_rows(kind)
            pltpu.make_async_copy(bounce[kind], gath[kind].at[l, pl.ds(pl.multiple_of(f * r, 8), r), :], loc.at[kind]).wait()
    load_x.wait()
    load_v.wait()

    def start_group(grp):
        own_d2d(grp)
        run(grp, 0, SUB)
        run(grp, SUB, SUB + 2)
        await_group(grp - 1)

    qkv0_n, qkv0_u, qkv0_s = mm_unit((0, QKV), h, qkv_epi(0))
    out0_n, out0_u, out0_s = mm_unit((0, OUT), h, out_epi(0))
    up0_n, up0_u, up0_s = mm_unit((0, UP), h, up_epi(0))
    down0_n, down0_u, down0_s = mm_unit((0, DOWN), g, down_epi(0, gath[DOWN].shape[1] // kt))
    qkv1_n, qkv1_u, qkv1_s = mm_unit((1, QKV), h, qkv_epi(1))
    out1_n, out1_u, out1_s = mm_unit((1, OUT), h, out_epi(1))
    up1_n, up1_u, up1_s = mm_unit((1, UP), h, up_epi(1))
    at_n, at_u = attn_unit()

    run(0, 0, SUB)
    run(0, SUB, 13)
    build_vectors()
    run(0, 13, ticks, *ln_unit(0, LN1_S, LN1_B))

    def begin(s):
        if COMPUTE:
            s()

    start_group(1)
    begin(qkv0_s)
    run(1, 5, 12, qkv0_n, qkv0_u)
    run(1, 12, ticks, at_n, at_u)

    start_group(2)
    begin(out0_s)
    run(2, 5, 8, out0_n, out0_u)
    begin(up0_s)
    run(2, 8, 9, *ln_unit(0, LN2_S, LN2_B))
    run(2, 9, ticks, up0_n, up0_u)

    start_group(3)
    begin(down0_s)
    run(3, 5, 19, down0_n, down0_u)
    run(3, 19, ticks, *ln_unit(1, LN1_S, LN1_B))

    start_group(4)
    begin(qkv1_s)
    run(4, 5, 11, qkv1_n, qkv1_u)
    run(4, 11, 17, at_n, at_u)
    begin(out1_s)
    run(4, 17, 20, out1_n, out1_u)
    run(4, 20, ticks, *ln_unit(1, LN2_S, LN2_B))

    start_group(5)
    begin(up1_s)
    run(5, 5, 15, up1_n, up1_u)
    acc[...] = jnp.zeros_like(acc)
    slot_ready(0)

    def slots(u):
        slot_wait(u)
        slot_ready(u + 1)
        slot_compute(u)

    if not COMPUTE:
        slot_wait(0)
    run(5, 15, ticks, steps - 1, slots)
    if COMPUTE:
        for j in range(SUB):
            xy_arrive(5, steps, j)
            if j == 0:
                slot_wait(steps - 1)
                slot_compute(steps - 1)
        slot_ready(steps)
        slot_wait(steps)
        slot_compute(steps)
    else:
        for j in range(SUB):
            xy_arrive(5, steps, j)
        for t in range(1, steps + 1):
            slot_ready(t)
            slot_wait(t)
    for mb in range(mblocks):
        msl = pl.ds(mb * mrows, mrows)
        x[msl, :] = (x[msl, :].astype(F32) + (acc[msl, :] + vec(1, B_DOWN, 0, width))).astype(BF16)
        pltpu.make_async_copy(x.at[msl], out_ref.at[msl], out_sem.at[mb]).start()
    for w in [w for grp in GROUPS for w in grp]:
        for sem in (snd_a, snd_b, snd_x, snd_y):
            wait_bytes(amount(w, steps), sem.at[wid(w)])
        wait_bytes(amount(w, 4 * nz), snd_d.at[wid(w)])
    wait_bytes(vecg.at[pl.ds(0, nz // 2)], snd_v.at[0])
    wait_bytes(vecg.at[pl.ds(0, nz // 2 - 1)], snd_v.at[1])
    wait_bytes(vecg.at[pl.ds(0, nz)], snd_v.at[2])
    for mb in range(mblocks):
        msl = pl.ds(mb * mrows, mrows)
        pltpu.make_async_copy(x.at[msl], out_ref.at[msl], out_sem.at[mb]).wait()


def solution(mesh):
    batch_spec = P(('dp', 'fsdp'), None, None)
    vector_spec = P(None, 'fsdp')
    matrix_spec = P(None, 'fsdp', None)
    in_specs = (batch_spec, vector_spec, vector_spec, P(None, 'fsdp', None, None, None), vector_spec, matrix_spec, vector_spec,
                vector_spec, vector_spec, matrix_spec, vector_spec, matrix_spec, vector_spec)
    nd = mesh.shape['fsdp']
    nz = nd // CORES
    ny = math.isqrt(mesh.shape['dp'])

    def local(images, ln1_s, ln1_b, w_qkv, b_qkv, w_out, b_out, ln2_s, ln2_b, w_up, b_up, w_down, b_down):
        nimg, seq, width = images.shape
        layers = w_qkv.shape[0]
        heads, hd = w_qkv.shape[3], w_qkv.shape[4]
        rows = nimg * seq
        x = images.reshape(rows, width)
        wq = w_qkv.reshape(layers, w_qkv.shape[1], 3 * width)
        vw = 4 * b_qkv.shape[1]
        pos = lax.rem(lax.axis_index('fsdp'), 4)
        lane = jnp.arange(vw)

        def place(v):
            n = v.shape[1]
            return jnp.where(lane // n == pos, jnp.tile(v, (1, vw // n)), jnp.zeros((), v.dtype))

        plain = jnp.pad(b_up, ((0, 0), (0, vw - b_up.shape[1])))
        vecs = jnp.stack([place(ln1_s), place(ln1_b), place(b_qkv), place(b_out), place(ln2_s), place(ln2_b), plain, place(b_down)], axis=1)
        vecs = vecs.reshape(layers * 8, vw)
        mats = (wq, w_out, w_up, w_down)
        any_spec = pl.BlockSpec(memory_space=pl.ANY)
        dma = pltpu.SemaphoreType.DMA
        nw = 4 * layers
        gshapes = [jax.ShapeDtypeStruct((layers, nd * m.shape[1], m.shape[2]), BF16) for m in mats]
        outs = pl.pallas_call(
            functools.partial(_kernel, (ny, nz, heads, hd)),
            out_shape=[jax.ShapeDtypeStruct((rows, width), BF16)] + gshapes,
            in_specs=[any_spec] * 6,
            out_specs=[any_spec] * 5,
            scratch_shapes=[
                pltpu.VMEM((rows, width), BF16),
                pltpu.VMEM((rows, width), BF16),
                pltpu.VMEM((rows, 3 * width), BF16),
                pltpu.VMEM((rows, w_up.shape[2]), BF16),
                pltpu.VMEM((rows, width), F32),
                pltpu.VMEM((2, width, width // 2), BF16),
                *[pltpu.VMEM(m.shape[1:], BF16) for m in mats],
                pltpu.VMEM((nd, layers * 8, vw), BF16),
                pltpu.VMEM((layers * 8, w_up.shape[2]), F32),
                *[dma((nw, nz - 1, SUB))] * 4,
                dma((nw,)),
                dma((nz,)),
                *[dma((nw,))] * 5,
                dma((3,)),
                dma((nz // 2,)),
                dma((nz // 2,)),
                dma,
                dma((4,)),
                dma((2,)),
                dma((3,)),
            ],
            compiler_params=pltpu.CompilerParams(collective_id=0, has_side_effects=True, vmem_limit_bytes=60 * 1024 * 1024),
        )(x, vecs, *mats)
        return outs[0].reshape(nimg, seq, width)

    return jax.shard_map(local, mesh=mesh, in_specs=in_specs, out_specs=batch_spec, check_vma=False)
```

```python
import functools
import math

import jax
import jax.numpy as jnp
from jax import lax
from jax.experimental import pallas as pl
from jax.experimental.pallas import tpu as pltpu
from jax.sharding import PartitionSpec as P

LN_EPS = 1e-6
GELU_C = math.sqrt(2.0 / math.pi)
MESH = pl.DeviceIdType.MESH
CORES = 2
SUB = 3
COMPUTE = True

LN1_S, LN1_B, B_QKV, B_OUT, LN2_S, LN2_B, B_UP, B_DOWN = range(8)
QKV, OUT, UP, DOWN = range(4)
GROUPS = (((0, QKV), (0, OUT)), ((0, UP),), ((0, DOWN),), ((1, QKV), (1, OUT)), ((1, UP),), ((1, DOWN),))
F32 = jnp.float32
BF16 = jnp.bfloat16


def _pack(ins, out):
    pos = lax.rem(lax.axis_index('fsdp'), 4)
    out[...] = jnp.zeros_like(out)
    for k, ref in enumerate(ins):
        n = ref.shape[1]
        if k == B_UP:
            out[2 * k:2 * k + 2, :n] = ref[...]
            continue
        src = lax.broadcasted_iota(jnp.int32, (n, 4 * n), 0)
        dst = lax.broadcasted_iota(jnp.int32, (n, 4 * n), 1)
        pick = (dst == src + pos * n).astype(BF16)
        out[2 * k:2 * k + 2, :4 * n] = jnp.dot(ref[...], pick, preferred_element_type=F32).astype(BF16)


def _kernel(dims, x_in, *refs):
    ny, nz, heads, hd = dims
    vin, win, refs = refs[:8], refs[8:12], refs[12:]
    out_ref, vec_in, refs = refs[0], refs[1], refs[2:]
    gath, refs = refs[:4], refs[4:]
    x, h, qkv, g, acc, wt, wl = refs[:7]
    bounce, refs = refs[7:11], refs[11:]
    vecg, vrow, vown, raw, raw32 = refs[:5]
    (rec_a, rec_b, rec_x, rec_y, rec_d, rec_l, snd_a, snd_b, snd_x, snd_y, snd_d, snd_v, vec_a, vec_b, vec_d, loc, tile_sem,
     out_sem) = refs[5:]

    rows, width = x.shape
    mblocks = 3
    mrows = rows // mblocks
    steps = nz - 1
    ticks = steps * SUB

    d = lax.axis_index('dp')
    f = lax.axis_index('fsdp')
    z, c = f // CORES, f % CORES
    up_dev = (d, ((z + 1) % nz) * CORES + c)
    dn_dev = (d, ((z + nz - 1) % nz) * CORES + c)
    sib_dev = (d, z * CORES + (CORES - 1 - c))
    x_dev = (d + ny * (1 - 2 * ((d // ny) % 2)), f)
    y_dev = (d + 1 - 2 * (d % 2), f)
    par = (d // ny + d % ny) % 2
    qa, qb = 2 * par, 2 * par + 1
    qx, qy = 2 * (1 - par), 2 * (1 - par) + 1

    def remote(src, dst, ssem, rsem, dev):
        return pltpu.make_async_remote_copy(src_ref=src, dst_ref=dst, send_sem=ssem, recv_sem=rsem, device_id=dev,
                                            device_id_type=MESH)

    def wid(w):
        return w[0] * 4 + w[1]

    def shard_rows(kind):
        return win[kind].shape[1]

    def part(ref, w, origin, q, j):
        l, kind = w
        r = shard_rows(kind)
        if kind == DOWN:
            n = r // SUB
            cols = ref.shape[2] // 4
            return ref.at[l, pl.ds(pl.multiple_of(origin * r + j * n, 8), n), pl.ds(pl.multiple_of(q * cols, 128), cols)]
        n = r // (4 * SUB)
        return ref.at[l, pl.ds(pl.multiple_of(origin * r + q * (r // 4) + j * n, 8), n), :]

    def quarter(ref, w, origin, q):
        l, kind = w
        r = shard_rows(kind)
        if kind == DOWN:
            cols = ref.shape[2] // 4
            return ref.at[l, pl.ds(pl.multiple_of(origin * r, 8), r), pl.ds(pl.multiple_of(q * cols, 128), cols)]
        return ref.at[l, pl.ds(pl.multiple_of(origin * r + q * (r // 4), 8), r // 4), :]

    def to_sibling(w, t, origin, q):
        p = quarter(gath[w[1]], w, origin, q)
        remote(p, p, snd_d.at[wid(w)], d2d_sem(w, t), sib_dev).start()

    def amount(w, quarters):
        l, kind = w
        r, cols = shard_rows(kind), gath[kind].shape[2]
        if kind == DOWN and quarters % 4:
            return gath[kind].at[l, pl.ds(0, quarters * r), pl.ds(0, cols // 4)]
        return gath[kind].at[l, pl.ds(0, quarters * (r // 4)), :]

    def wait_bytes(view, sem):
        pltpu.make_async_copy(view, view, sem).wait()

    def d2d_sem(w, t):
        return rec_l.at[t] if w == GROUPS[-1][-1] else rec_d.at[wid(w)]

    def own_send(grp, j, kinds=(QKV, OUT, UP, DOWN)):
        for w in GROUPS[grp]:
            l, kind = w
            if kind not in kinds:
                continue
            for q, snd, rec, dev in ((qa, snd_a, rec_a, up_dev), (qb, snd_b, rec_b, dn_dev)):
                dst = part(gath[kind], w, f, q, j)
                src = dst if kind == QKV else part(win[kind], w, 0, q, j)
                remote(src, dst, snd.at[wid(w)], rec.at[wid(w), 0, j], dev).start()

    def own_d2d(grp):
        for w in GROUPS[grp]:
            l, kind = w
            r = shard_rows(kind)
            dst = gath[kind].at[l, pl.ds(pl.multiple_of(f * r, 8), r), :]
            remote(dst if kind == QKV else win[kind].at[l], dst, snd_d.at[wid(w)], d2d_sem(w, 0), sib_dev).start()

    def xy_arrive(grp, t, j):
        oa = ((z - t + nz) % nz) * CORES + c
        ob = ((z + t) % nz) * CORES + c
        for w in GROUPS[grp]:
            l, kind = w
            px, py = part(gath[kind], w, oa, qx, j), part(gath[kind], w, ob, qy, j)
            remote(px, px, snd_x.at[wid(w)], rec_x.at[wid(w), t - 1, j], x_dev).wait_recv()
            remote(px, px, snd_d.at[wid(w)], d2d_sem(w, t), sib_dev).start()
            remote(py, py, snd_y.at[wid(w)], rec_y.at[wid(w), t - 1, j], y_dev).wait_recv()
            remote(py, py, snd_d.at[wid(w)], d2d_sem(w, t), sib_dev).start()

    def tick(grp, i, early):
        t, j = i // SUB + 1, i % SUB
        oa = ((z - t + nz) % nz) * CORES + c
        ob = ((z + t) % nz) * CORES + c
        for w in GROUPS[grp]:
            l, kind = w
            for o, q, snd, rec, dev in ((oa, qa, snd_a, rec_a, up_dev), (ob, qb, snd_b, rec_b, dn_dev)):
                p = part(gath[kind], w, o, q, j)
                remote(p, p, snd.at[wid(w)], rec.at[wid(w), t - 1, j], dev).wait_recv()

                @pl.when(t < steps)
                def _():
                    remote(p, p, snd.at[wid(w)], rec.at[wid(w), t, j], dev).start()

            pa, pb = part(gath[kind], w, oa, qa, j), part(gath[kind], w, ob, qb, j)
            remote(pa, pa, snd_x.at[wid(w)], rec_x.at[wid(w), t - 1, j], x_dev).start()
            remote(pb, pb, snd_y.at[wid(w)], rec_y.at[wid(w), t - 1, j], y_dev).start()
        if grp + 1 < len(GROUPS):

            @pl.when(t == steps - 1)
            def _():
                own_send(grp + 1, j)

        if grp == 0:
            half = nz // 2
            va, vb = vecg.at[oa], vecg.at[ob]

            @pl.when(jnp.logical_and(j == 0, t <= half))
            def _():
                remote(va, va, snd_v.at[0], vec_a.at[t - 1], up_dev).wait_recv()

                @pl.when(t < half)
                def _():
                    remote(va, va, snd_v.at[0], vec_a.at[t], up_dev).start()

                remote(va, va, snd_v.at[2], vec_d, sib_dev).start()

            @pl.when(jnp.logical_and(j == 0, t < half))
            def _():
                remote(vb, vb, snd_v.at[1], vec_b.at[t - 1], dn_dev).wait_recv()

                @pl.when(t < half - 1)
                def _():
                    remote(vb, vb, snd_v.at[1], vec_b.at[t], dn_dev).start()

                remote(vb, vb, snd_v.at[2], vec_d, sib_dev).start()

        if not early:
            xy_arrive(grp, t - 1, j)
        elif grp > 0:
            xy_arrive(grp - 1, steps, j)

        @pl.when(j == SUB - 1)
        def _():
            for w in GROUPS[grp]:
                to_sibling(w, t, oa, qa)
                to_sibling(w, t, ob, qb)

    def run(grp, lo, hi, total=0, unit=None):
        def body(i, carry):
            tick(grp, i, hi <= SUB)
            if unit is not None and COMPUTE:
                k = i - lo
                lax.fori_loop((k * total) // (hi - lo), ((k + 1) * total) // (hi - lo), lambda u, cc: (unit(u), cc)[1], 0)
            return carry

        lax.fori_loop(lo, hi, body, 0)

    def await_group(grp):
        for w in GROUPS[grp]:
            wait_bytes(amount(w, 4 * nz), rec_d.at[wid(w)])

    def vec(l, k, n, width_):
        return vrow[pl.ds(2 * k + l, 1), pl.ds(n, width_)]

    def ln_unit(l, ks, kb):
        n = 64

        def unit(u):
            sl = pl.ds(pl.multiple_of(u * n, n), n)
            v = x[sl, :].astype(F32)
            v = v - jnp.mean(v, axis=-1, keepdims=True)
            var = jnp.mean(v * v, axis=-1, keepdims=True)
            y = v * lax.rsqrt(var + LN_EPS)
            h[sl, :] = (y * vec(l, ks, 0, width) + vec(l, kb, 0, width)).astype(BF16)

        return rows // n, unit

    kt, nt = wt.shape[1], wt.shape[2]
    nu = nt // 2

    def tile_copies(w, i):
        l, kind = w
        ref, dst, sem = gath[kind].at[l], wt.at[i % 2], tile_sem.at[i % 2]
        if kind != DOWN:
            return [pltpu.make_async_copy(ref.at[:, pl.ds(pl.multiple_of(i * nt, 128), nt)], dst, sem)]
        n, k = i // 2, i % 2
        return [
            pltpu.make_async_copy(
                ref.at[pl.ds(pl.multiple_of((2 * k + s) * kt, 8), kt), pl.ds(pl.multiple_of(n * nu, 128), nu)],
                dst.at[:, pl.ds(s * nu, nu)], sem) for s in range(2)
        ]

    def tile_start(w, i):
        for cp in tile_copies(w, i):
            cp.start()

    def tile_wait(i):
        pltpu.make_async_copy(wt.at[i % 2], wt.at[i % 2], tile_sem.at[i % 2]).wait()

    def mm_unit(w, a_ref, epilogue):
        l, kind = w
        ntiles = gath[kind].shape[2] // nt if kind != DOWN else 2 * (gath[kind].shape[2] // nu)

        def unit(i):
            tile_wait(i)

            @pl.when(i + 1 < ntiles)
            def _():
                tile_start(w, i + 1)

            if kind == DOWN:
                n, k = i // 2, i % 2
                n0 = pl.multiple_of(n * nu, 128)
                res = sum(
                    jnp.dot(a_ref[:, pl.ds(pl.multiple_of((2 * k + s) * kt, 128), kt)], wt[i % 2, :, s * nu:(s + 1) * nu],
                            preferred_element_type=F32) for s in range(2))
                epilogue(res, pl.ds(n0, nu), n0, k)
                return
            for s in range(nt // nu):
                n0 = pl.multiple_of(i * nt + s * nu, 128)
                res = jnp.dot(a_ref[...], wt[i % 2, :, s * nu:(s + 1) * nu], preferred_element_type=F32)
                epilogue(res, pl.ds(n0, nu), n0, 0)

        return ntiles, unit, lambda: tile_start(w, 0)

    def gelu_tanh(v):
        half = 0.5 * v
        return half + half * jnp.tanh(v * (GELU_C + (GELU_C * 0.044715) * (v * v)))

    def qkv_epi(l):
        def epi(res, nsl, n0, k):
            qkv[:, nsl] = (res + vec(l, B_QKV, n0, nu)).astype(BF16)

        return epi

    def out_epi(l):
        def epi(res, nsl, n0, k):
            x[:, nsl] = (x[:, nsl].astype(F32) + (res + vec(l, B_OUT, n0, nu))).astype(BF16)

        return epi

    def up_epi(l):
        def epi(res, nsl, n0, k):
            g[:, nsl] = gelu_tanh(res + vec(l, B_UP, n0, nu)).astype(BF16)

        return epi

    def down_epi(l):
        def epi(res, nsl, n0, k):
            @pl.when(k == 0)
            def _():
                acc[:, nsl] = res

            @pl.when(k == 1)
            def _():
                x[:, nsl] = (x[:, nsl].astype(F32) + (acc[:, nsl] + res + vec(l, B_DOWN, n0, nu))).astype(BF16)

        return epi

    seq = 2 * 128
    hg = 4

    def attn_unit():
        lane = lax.broadcasted_iota(jnp.int32, (1, seq), 1)
        gw = hg * hd
        scale = hd ** -0.5 * math.log2(math.e)

        def window(q2, k2, v2, offs):
            ms = [jnp.logical_and(lane >= o, lane < o + hd).astype(BF16) for o in offs]
            ks = jnp.concatenate([k2 * m for m in ms], axis=0)
            vs = jnp.concatenate([v2 * m for m in ms], axis=0)
            s = lax.dot_general(q2, ks, (((1,), (1,)), ((), ())), preferred_element_type=F32)
            ps = []
            for i in range(len(offs)):
                si = s[:, i * seq:(i + 1) * seq]
                e = jnp.exp2((si - jnp.max(si, axis=-1, keepdims=True)) * scale)
                ps.append((e * (1.0 / jnp.sum(e, axis=-1, keepdims=True))).astype(BF16))
            return jnp.dot(jnp.concatenate(ps, axis=1), vs, preferred_element_type=F32)

        def unit(u):
            img, grp = u // (heads // hg), u % (heads // hg)
            msl = pl.ds(pl.multiple_of(img * seq, seq), seq)

            def win_(base, off):
                return qkv[msl, pl.ds(pl.multiple_of(base * width + grp * gw + off, 128), seq)]

            o0 = window(win_(0, 0), win_(1, 0), win_(2, 0), (0, hd))
            o1 = window(win_(0, 128), win_(1, 128), win_(2, 128), (2 * hd - 128, 3 * hd - 128))
            c0 = grp * gw
            h[msl, pl.ds(pl.multiple_of(c0, 128), 128)] = o0[:, :128].astype(BF16)
            h[msl, pl.ds(pl.multiple_of(c0 + 128, 128), 128)] = (o0[:, 128:] + o1[:, :128]).astype(BF16)
            h[msl, pl.ds(pl.multiple_of(c0 + 256, 128), 128)] = o1[:, 128:].astype(BF16)

        return (rows // seq) * (heads // hg), unit

    def build_vectors():
        wait_bytes(vecg.at[pl.ds(0, nz)], vec_d)
        nd = nz * CORES
        for a in range(nd // 4):
            s = vecg[4 * a].astype(F32)
            for r in range(1, 4):
                s = s + vecg[4 * a + r].astype(F32)
            for l in range(2):
                for k in (LN1_S, LN1_B, B_OUT, LN2_S, LN2_B, B_DOWN):
                    wv = width // (nd // 4)
                    vrow[2 * k + l:2 * k + l + 1, a * wv:(a + 1) * wv] = s[2 * k + l:2 * k + l + 1, :wv]
                wv = 3 * width // (nd // 4)
                vrow[2 * B_QKV + l:2 * B_QKV + l + 1, a * wv:(a + 1) * wv] = s[2 * B_QKV + l:2 * B_QKV + l + 1, :wv]
        wv = vrow.shape[1] // nd
        for o in range(nd):
            s = vecg[o].astype(F32)
            for l in range(2):
                vrow[2 * B_UP + l:2 * B_UP + l + 1, o * wv:(o + 1) * wv] = s[2 * B_UP + l:2 * B_UP + l + 1, :wv]

    last = GROUPS[-1][-1]
    zrows = CORES * win[DOWN].shape[1]
    dq = width // 4

    def slot_copies(t):
        za, zb = (z - t + nz) % nz, (z + t) % nz
        for n, (zz, q, r0, c0) in enumerate(((za, 0, 0, 0), (za, 2, 0, dq), (zb, 1, zrows, 0), (zb, 3, zrows, dq))):
            yield pltpu.make_async_copy(
                gath[DOWN].at[last[0], pl.ds(pl.multiple_of(zz * zrows, 8), zrows), pl.ds(q * dq, dq)],
                wl.at[t % 2, pl.ds(r0, zrows), pl.ds(c0, dq)], tile_sem.at[t % 2])

    def slot_ready(t):
        l, kind = last
        wait_bytes(gath[kind].at[l, pl.ds(0, win[kind].shape[1]), :], rec_l.at[t])
        for cp in slot_copies(t):
            cp.start()

    def slot_wait(t):
        pltpu.make_async_copy(wl.at[t % 2], wl.at[t % 2], tile_sem.at[t % 2]).wait()

    def slot_compute(t):
        za, zb = (z - t + nz) % nz, (z + t) % nz

        for zz, r0, c0 in ((za, 0, 0), (zb, zrows, 2 * dq)):
            for nn in range(2 * dq // nu):
                csl = slice(c0 + nn * nu, c0 + (nn + 1) * nu)
                acc[:, csl] += jnp.dot(g[:, pl.ds(pl.multiple_of(zz * zrows, 128), zrows)],
                                       wl[t % 2, r0:r0 + zrows, nn * nu:(nn + 1) * nu], preferred_element_type=F32)

    vec_mine = vecg.at[f]
    load_x = pltpu.make_async_copy(x_in, x, out_sem.at[0])
    load_v = pltpu.make_async_copy(vec_in, vec_mine, out_sem.at[1])

    def own_load(kind):
        return pltpu.make_async_copy(win[kind], bounce[kind], loc.at[kind])

    def own_store(l, kind):
        r = shard_rows(kind)
        return pltpu.make_async_copy(bounce[kind].at[l], gath[kind].at[l, pl.ds(pl.multiple_of(f * r, 8), r), :], loc.at[4 * (l + 1) + kind])

    def load_raw(l):
        return pltpu.make_async_copy(win[QKV].at[l], raw, loc.at[QKV])

    def relayout(l, first, r):
        nh = raw.shape[1]
        wide, groups = r // 8, nh // hg

        def unit(u):
            @pl.when(u < wide)
            def _():
                raw32[pl.ds(pl.multiple_of(u * 8 * nh, 8), 8 * nh), :] = raw[pl.ds(pl.multiple_of(first + u * 8, 8), 8)].astype(F32).reshape(8 * nh, hd)

            @pl.when(u >= wide)
            def _():
                i = u - wide
                src = lax.broadcasted_iota(jnp.int32, (hd, hg * hd), 0)
                dst = lax.broadcasted_iota(jnp.int32, (hd, hg * hd), 1)
                res = sum(
                    jnp.dot(raw32[pl.ds(hg * i + k, r, stride=nh), :].astype(BF16), (dst == src + k * hd).astype(BF16),
                            preferred_element_type=F32) for k in range(hg))
                bounce[QKV][l, pl.ds(pl.multiple_of(first, 8), r), pl.ds(pl.multiple_of(i * hg * hd, 128), hg * hd)] = res.astype(BF16)

        return wide + groups, unit

    load_raw(0).start()
    load_x.start()
    for kind in (OUT, UP, DOWN):
        own_load(kind).start()
    barrier = pltpu.get_barrier_semaphore()
    for dev in (up_dev, dn_dev, sib_dev, x_dev, y_dev):
        pl.semaphore_signal(barrier, inc=1, device_id=dev, device_id_type=MESH)
    half_rows = raw.shape[0] // 2
    mine, other = par * half_rows, (1 - par) * half_rows

    def half_store(first):
        r = shard_rows(QKV)
        return pltpu.make_async_copy(bounce[QKV].at[0, pl.ds(pl.multiple_of(first, 8), half_rows)],
                                     gath[QKV].at[0, pl.ds(pl.multiple_of(f * r + first, 8), half_rows), :], loc.at[4 + QKV])

    def relay_half(first):
        n_re, re0 = relayout(0, first, half_rows)
        lax.fori_loop(0, n_re, lambda u, cc: (re0(u), cc)[1], 0)
        half_store(first).start()

    pl.semaphore_wait(barrier, 5)
    for j in range(SUB):
        own_send(0, j, (OUT,))
    load_raw(0).wait()
    relay_half(mine)
    _pack(vin, vown)
    save_v = pltpu.make_async_copy(vown, vec_in, out_sem.at[1])
    save_v.start()
    half_store(mine).wait()
    for j in range(SUB):
        own_send(0, j, (QKV,))
    save_v.wait()
    remote(vec_in, vec_mine, snd_v.at[0], vec_a.at[0], up_dev).start()
    remote(vec_in, vec_mine, snd_v.at[1], vec_b.at[0], dn_dev).start()
    load_v.start()
    relay_half(other)
    load_raw(1).start()
    half_store(other).wait()
    remote(vec_in, vec_mine, snd_v.at[2], vec_d, sib_dev).start()
    own_d2d(0)
    for kind in (OUT, UP, DOWN):
        own_load(kind).wait()
        for l in range(2):
            own_store(l, kind).start()

    def start_group(grp, first=(), second=()):
        run(grp, 0, SUB, *first)
        run(grp, SUB, SUB + 1, *second)
        await_group(grp - 1)
        own_d2d(grp)

    qkv0_n, qkv0_u, qkv0_s = mm_unit((0, QKV), h, qkv_epi(0))
    out0_n, out0_u, out0_s = mm_unit((0, OUT), h, out_epi(0))
    up0_n, up0_u, up0_s = mm_unit((0, UP), h, up_epi(0))
    down0_n, down0_u, down0_s = mm_unit((0, DOWN), g, down_epi(0))
    qkv1_n, qkv1_u, qkv1_s = mm_unit((1, QKV), h, qkv_epi(1))
    out1_n, out1_u, out1_s = mm_unit((1, OUT), h, out_epi(1))
    up1_n, up1_u, up1_s = mm_unit((1, UP), h, up_epi(1))
    at_n, at_u = attn_unit()

    def begin(s):
        if COMPUTE:
            s()

    run(0, 0, SUB)
    load_raw(1).wait()
    run(0, SUB, 13, *relayout(1, 0, raw.shape[0]))
    own_store(1, QKV).start()
    run(0, 13, 14)
    load_v.wait()
    load_x.wait()
    for kind in range(4):
        for l in range(2):
            if (l, kind) != (0, QKV):
                own_store(l, kind).wait()
    build_vectors()
    run(0, 14, ticks, *ln_unit(0, LN1_S, LN1_B))

    start_group(1)
    begin(qkv0_s)
    run(1, 4, 13, qkv0_n, qkv0_u)
    run(1, 13, ticks, at_n, at_u)

    begin(out0_s)
    start_group(2, (2, out0_u), (out0_n - 2, lambda u: out0_u(u + 2)))
    begin(up0_s)
    run(2, 4, 7, *ln_unit(0, LN2_S, LN2_B))
    run(2, 7, ticks, up0_n, up0_u)

    start_group(3)
    begin(down0_s)
    run(3, 4, 17, down0_n, down0_u)
    run(3, 17, ticks, *ln_unit(1, LN1_S, LN1_B))
    acc[...] = jnp.zeros_like(acc)

    start_group(4)
    begin(qkv1_s)
    run(4, 4, 11, qkv1_n, qkv1_u)
    run(4, 11, 16, at_n, at_u)
    begin(out1_s)
    run(4, 16, 19, out1_n, out1_u)
    run(4, 19, ticks, *ln_unit(1, LN2_S, LN2_B))

    start_group(5)
    begin(up1_s)
    run(5, 4, 15, up1_n, up1_u)
    slot_ready(0)

    def slots(u):
        slot_wait(u)
        slot_ready(u + 1)
        slot_compute(u)

    if not COMPUTE:
        slot_wait(0)
    run(5, 15, ticks, steps - 1, slots)
    if COMPUTE:
        for j in range(SUB):
            xy_arrive(5, steps, j)
            if j == 0:
                slot_wait(steps - 1)
                slot_compute(steps - 1)
        slot_ready(steps)
        slot_wait(steps)
        slot_compute(steps)
    else:
        for j in range(SUB):
            xy_arrive(5, steps, j)
        for t in range(1, steps + 1):
            slot_ready(t)
            slot_wait(t)
    for mb in range(mblocks):
        msl = pl.ds(mb * mrows, mrows)
        for n, q in enumerate((0, 2, 1, 3)):
            csl = slice(q * dq, (q + 1) * dq)
            x[msl, csl] = (x[msl, csl].astype(F32) + (acc[msl, n * dq:(n + 1) * dq] + vec(1, B_DOWN, q * dq, dq))).astype(BF16)
        pltpu.make_async_copy(x.at[msl], out_ref.at[msl], out_sem.at[mb]).start()
    for w in [w for grp in GROUPS for w in grp]:
        for sem in (snd_a, snd_b, snd_x, snd_y):
            wait_bytes(amount(w, steps), sem.at[wid(w)])
        wait_bytes(amount(w, 4 * nz), snd_d.at[wid(w)])
    wait_bytes(vecg.at[pl.ds(0, nz // 2)], snd_v.at[0])
    wait_bytes(vecg.at[pl.ds(0, nz // 2 - 1)], snd_v.at[1])
    wait_bytes(vecg.at[pl.ds(0, nz)], snd_v.at[2])
    for mb in range(mblocks):
        msl = pl.ds(mb * mrows, mrows)
        pltpu.make_async_copy(x.at[msl], out_ref.at[msl], out_sem.at[mb]).wait()


def solution(mesh):
    batch_spec = P(('dp', 'fsdp'), None, None)
    vector_spec = P(None, 'fsdp')
    matrix_spec = P(None, 'fsdp', None)
    in_specs = (batch_spec, vector_spec, vector_spec, P(None, 'fsdp', None, None, None), vector_spec, matrix_spec, vector_spec,
                vector_spec, vector_spec, matrix_spec, vector_spec, matrix_spec, vector_spec)
    nd = mesh.shape['fsdp']
    nz = nd // CORES
    ny = math.isqrt(mesh.shape['dp'])

    def local(images, ln1_s, ln1_b, w_qkv, b_qkv, w_out, b_out, ln2_s, ln2_b, w_up, b_up, w_down, b_down):
        nimg, seq, width = images.shape
        layers = w_qkv.shape[0]
        heads, hd = w_qkv.shape[3], w_qkv.shape[4]
        rows = nimg * seq
        x = images.reshape(rows, width)
        vw = 4 * b_qkv.shape[1]
        vecs = (ln1_s, ln1_b, b_qkv, b_out, ln2_s, ln2_b, b_up, b_down)
        mats = (w_qkv.reshape(layers, w_qkv.shape[1], 3 * heads, hd), w_out, w_up, w_down)
        cols = (3 * width, width, w_up.shape[2], width)
        any_spec = pl.BlockSpec(memory_space=pl.ANY)
        dma = pltpu.SemaphoreType.DMA
        nw = 4 * layers
        gshapes = [jax.ShapeDtypeStruct((layers, nd * m.shape[1], n), BF16) for m, n in zip(mats, cols)]
        outs = pl.pallas_call(
            functools.partial(_kernel, (ny, nz, heads, hd)),
            out_shape=[jax.ShapeDtypeStruct((rows, width), BF16), jax.ShapeDtypeStruct((layers * 8, vw), BF16)] + gshapes,
            in_specs=[any_spec] + [pl.BlockSpec(memory_space=pltpu.VMEM)] * 8 + [any_spec] * 4,
            out_specs=[any_spec] * 6,
            scratch_shapes=[
                pltpu.VMEM((rows, width), BF16),
                pltpu.VMEM((rows, width), BF16),
                pltpu.VMEM((rows, 3 * width), BF16),
                pltpu.VMEM((rows, w_up.shape[2]), BF16),
                pltpu.VMEM((rows, width), F32),
                pltpu.VMEM((2, width, width // 3), BF16),
                pltpu.VMEM((2, width, width // 2), BF16),
                *[pltpu.VMEM((*m.shape[:2], n), BF16) for m, n in zip(mats, cols)],
                pltpu.VMEM((nd, layers * 8, vw), BF16),
                pltpu.VMEM((layers * 8, w_up.shape[2]), F32),
                pltpu.VMEM((layers * 8, vw), BF16),
                pltpu.VMEM(mats[0].shape[1:], BF16),
                pltpu.VMEM((mats[0].shape[1] * 3 * heads, hd), F32),
                *[dma((nw, nz - 1, SUB))] * 4,
                dma((nw,)),
                dma((nz,)),
                *[dma((nw,))] * 5,
                dma((3,)),
                dma((nz // 2,)),
                dma((nz // 2,)),
                dma,
                dma((4 * (layers + 1),)),
                dma((2,)),
                dma((3,)),
            ],
            compiler_params=pltpu.CompilerParams(collective_id=0, has_side_effects=True, vmem_limit_bytes=56 * 1024 * 1024),
        )(x, *vecs, *mats)
        return outs[0].reshape(nimg, seq, width)

    return jax.shard_map(local, mesh=mesh, in_specs=in_specs, out_specs=batch_spec, check_vma=False)
```

```python
import functools
import math

import jax
import jax.numpy as jnp
from jax import lax
from jax.experimental import pallas as pl
from jax.experimental.pallas import tpu as pltpu
from jax.sharding import PartitionSpec as P

LN_EPS = 1e-6
COPIES = 8
GELU_C = math.sqrt(2.0 / math.pi)
MESH = pl.DeviceIdType.MESH
CORES = 2
SUB = 3
COMPUTE = True

LN1_S, LN1_B, B_QKV, B_OUT, LN2_S, LN2_B, B_UP, B_DOWN = range(8)
SEG_ROWS = 14
QKV, OUT, UP, DOWN = range(4)
GROUPS = (((0, QKV), (0, OUT)), ((0, UP),), ((0, DOWN),), ((1, QKV), (1, OUT)), ((1, UP),), ((1, DOWN),))
F32 = jnp.float32
BF16 = jnp.bfloat16


def _pack(ins, out):
    pos = lax.rem(lax.axis_index('fsdp'), 4)
    out[...] = jnp.zeros_like(out)
    for k, ref in enumerate(ins):
        n = ref.shape[1]
        if k == B_UP:
            out[2 * k:2 * k + 2, :n] = ref[...]
            continue
        src = lax.broadcasted_iota(jnp.int32, (n, 4 * n), 0)
        dst = lax.broadcasted_iota(jnp.int32, (n, 4 * n), 1)
        pick = (dst == src + pos * n).astype(BF16)
        res = jnp.dot(ref[...], pick, preferred_element_type=F32).astype(BF16)
        for seg in range(4 * n // out.shape[1]):
            row = 2 * k if seg == 0 else SEG_ROWS + 2 * seg
            out[row:row + 2, :] = res[:, seg * out.shape[1]:(seg + 1) * out.shape[1]]


def _kernel(dims, x_in, *refs):
    ny, nz, heads, hd = dims
    vin, win, refs = refs[:8], refs[8:12], refs[12:]
    out_ref, vec_in, refs = refs[0], refs[1], refs[2:]
    gath, refs = refs[:4], refs[4:]
    x, h, qkv, g, acc, wt, wl = refs[:7]
    bounce, refs = refs[7:11], refs[11:]
    vecg, vrow, vown, raw, raw32 = refs[:5]
    (rec_a, rec_b, rec_x, rec_y, rec_d, rec_l, snd_a, snd_b, snd_x, snd_y, snd_d, snd_v, vec_a, vec_b, vec_d, loc, tile_sem,
     out_sem) = refs[5:]

    rows, width = x.shape
    mblocks = 3
    mrows = rows // mblocks
    steps = nz - 1
    ticks = steps * SUB

    d = lax.axis_index('dp')
    f = lax.axis_index('fsdp')
    z, c = f // CORES, f % CORES
    up_dev = (d, ((z + 1) % nz) * CORES + c)
    dn_dev = (d, ((z + nz - 1) % nz) * CORES + c)
    sib_dev = (d, z * CORES + (CORES - 1 - c))
    x_dev = (d + ny * (1 - 2 * ((d // ny) % 2)), f)
    y_dev = (d + 1 - 2 * (d % 2), f)
    par = (d // ny + d % ny) % 2
    qa, qb = 2 * par, 2 * par + 1
    qx, qy = 2 * (1 - par), 2 * (1 - par) + 1

    def remote(src, dst, ssem, rsem, dev):
        return pltpu.make_async_remote_copy(src_ref=src, dst_ref=dst, send_sem=ssem, recv_sem=rsem, device_id=dev,
                                            device_id_type=MESH)

    def wid(w):
        return w[0] * 4 + w[1]

    def shard_rows(kind):
        return win[kind].shape[1]

    def part(ref, w, origin, q, j):
        l, kind = w
        r = shard_rows(kind)
        if kind == DOWN:
            n = r // SUB
            cols = ref.shape[2] // 4
            return ref.at[l, pl.ds(pl.multiple_of(origin * r + j * n, 8), n), pl.ds(pl.multiple_of(q * cols, 128), cols)]
        n = r // (4 * SUB)
        return ref.at[l, pl.ds(pl.multiple_of(origin * r + q * (r // 4) + j * n, 8), n), :]

    def quarter(ref, w, origin, q):
        l, kind = w
        r = shard_rows(kind)
        if kind == DOWN:
            cols = ref.shape[2] // 4
            return ref.at[l, pl.ds(pl.multiple_of(origin * r, 8), r), pl.ds(pl.multiple_of(q * cols, 128), cols)]
        return ref.at[l, pl.ds(pl.multiple_of(origin * r + q * (r // 4), 8), r // 4), :]

    def to_sibling(w, t, origin, q):
        p = quarter(gath[w[1]], w, origin, q)
        remote(p, p, snd_d.at[wid(w)], d2d_sem(w, t), sib_dev).start()

    def amount(w, quarters):
        l, kind = w
        r, cols = shard_rows(kind), gath[kind].shape[2]
        if kind == DOWN and quarters % 4:
            return gath[kind].at[l, pl.ds(0, quarters * r), pl.ds(0, cols // 4)]
        return gath[kind].at[l, pl.ds(0, quarters * (r // 4)), :]

    def wait_bytes(view, sem):
        pltpu.make_async_copy(view, view, sem).wait()

    def d2d_sem(w, t):
        return rec_l.at[t] if w == GROUPS[-1][-1] else rec_d.at[wid(w)]

    def own_send(grp, j, kinds=(QKV, OUT, UP, DOWN)):
        for w in GROUPS[grp]:
            l, kind = w
            if kind not in kinds:
                continue
            for q, snd, rec, dev in ((qa, snd_a, rec_a, up_dev), (qb, snd_b, rec_b, dn_dev)):
                dst = part(gath[kind], w, f, q, j)
                src = dst if kind == QKV else part(win[kind], w, 0, q, j)
                remote(src, dst, snd.at[wid(w)], rec.at[wid(w), 0, j], dev).start()

    def own_d2d(grp):
        for w in GROUPS[grp]:
            l, kind = w
            r = shard_rows(kind)
            dst = gath[kind].at[l, pl.ds(pl.multiple_of(f * r, 8), r), :]
            remote(dst if kind == QKV else win[kind].at[l], dst, snd_d.at[wid(w)], d2d_sem(w, 0), sib_dev).start()

    def xy_arrive(grp, t, j):
        oa = ((z - t + nz) % nz) * CORES + c
        ob = ((z + t) % nz) * CORES + c
        for w in GROUPS[grp]:
            l, kind = w
            px, py = part(gath[kind], w, oa, qx, j), part(gath[kind], w, ob, qy, j)
            remote(px, px, snd_x.at[wid(w)], rec_x.at[wid(w), t - 1, j], x_dev).wait_recv()
            remote(px, px, snd_d.at[wid(w)], d2d_sem(w, t), sib_dev).start()
            remote(py, py, snd_y.at[wid(w)], rec_y.at[wid(w), t - 1, j], y_dev).wait_recv()
            remote(py, py, snd_d.at[wid(w)], d2d_sem(w, t), sib_dev).start()

    def tick(grp, i, early):
        t, j = i // SUB + 1, i % SUB
        oa = ((z - t + nz) % nz) * CORES + c
        ob = ((z + t) % nz) * CORES + c
        for w in GROUPS[grp]:
            l, kind = w
            for o, q, snd, rec, dev in ((oa, qa, snd_a, rec_a, up_dev), (ob, qb, snd_b, rec_b, dn_dev)):
                p = part(gath[kind], w, o, q, j)
                remote(p, p, snd.at[wid(w)], rec.at[wid(w), t - 1, j], dev).wait_recv()

                @pl.when(t < steps)
                def _():
                    remote(p, p, snd.at[wid(w)], rec.at[wid(w), t, j], dev).start()

            pa, pb = part(gath[kind], w, oa, qa, j), part(gath[kind], w, ob, qb, j)
            remote(pa, pa, snd_x.at[wid(w)], rec_x.at[wid(w), t - 1, j], x_dev).start()
            remote(pb, pb, snd_y.at[wid(w)], rec_y.at[wid(w), t - 1, j], y_dev).start()
        if grp + 1 < len(GROUPS):

            @pl.when(jnp.logical_and(t == steps - 1, j >= (1 if grp == 0 else 0)))
            def _():
                own_send(grp + 1, j)

        if grp == 0:
            half = nz // 2
            va, vb = vecg.at[oa], vecg.at[ob]

            @pl.when(jnp.logical_and(j == 0, t <= half))
            def _():
                remote(va, va, snd_v.at[0], vec_a.at[t - 1], up_dev).wait_recv()

                @pl.when(t < half)
                def _():
                    remote(va, va, snd_v.at[0], vec_a.at[t], up_dev).start()

                remote(va, va, snd_v.at[2], vec_d, sib_dev).start()

            @pl.when(jnp.logical_and(j == 0, t < half))
            def _():
                remote(vb, vb, snd_v.at[1], vec_b.at[t - 1], dn_dev).wait_recv()

                @pl.when(t < half - 1)
                def _():
                    remote(vb, vb, snd_v.at[1], vec_b.at[t], dn_dev).start()

                remote(vb, vb, snd_v.at[2], vec_d, sib_dev).start()

        if not early:
            xy_arrive(grp, t - 1, j)
        elif grp > 0:
            xy_arrive(grp - 1, steps, j)

        @pl.when(j == SUB - 1)
        def _():
            for w in GROUPS[grp]:
                to_sibling(w, t, oa, qa)
                to_sibling(w, t, ob, qb)

    def run(grp, lo, hi, total=0, unit=None):
        def body(i, carry):
            tick(grp, i, hi <= SUB)
            if unit is not None and COMPUTE:
                k = i - lo
                lax.fori_loop((k * total) // (hi - lo), ((k + 1) * total) // (hi - lo), lambda u, cc: (unit(u), cc)[1], 0)
            return carry

        lax.fori_loop(lo, hi, body, 0)

    def await_group(grp):
        for w in GROUPS[grp]:
            wait_bytes(amount(w, 4 * nz), rec_d.at[wid(w)])

    def vec(l, k, n, width_):
        return vrow[pl.ds(2 * k + l, 1), pl.ds(n, width_)]

    def ln_unit(l, ks, kb):
        n = 64

        def unit(u):
            sl = pl.ds(pl.multiple_of(u * n, n), n)
            v = x[sl, :].astype(F32)
            v = v - jnp.mean(v, axis=-1, keepdims=True)
            var = jnp.mean(v * v, axis=-1, keepdims=True)
            y = v * lax.rsqrt(var + LN_EPS)
            h[sl, :] = (y * vec(l, ks, 0, width) + vec(l, kb, 0, width)).astype(BF16)

        return rows // n, unit

    kt, nt = wt.shape[1], wt.shape[2]
    nu = nt // 2

    def tile_copies(w, i):
        l, kind = w
        ref, dst, sem = gath[kind].at[l], wt.at[i % 2], tile_sem.at[i % 2]
        if kind != DOWN:
            return [pltpu.make_async_copy(ref.at[:, pl.ds(pl.multiple_of(i * nt, 128), nt)], dst, sem)]
        n, k = i // 2, i % 2
        return [
            pltpu.make_async_copy(
                ref.at[pl.ds(pl.multiple_of((2 * k + s) * kt, 8), kt), pl.ds(pl.multiple_of(n * nu, 128), nu)],
                dst.at[:, pl.ds(s * nu, nu)], sem) for s in range(2)
        ]

    def tile_start(w, i):
        for cp in tile_copies(w, i):
            cp.start()

    def tile_wait(i):
        pltpu.make_async_copy(wt.at[i % 2], wt.at[i % 2], tile_sem.at[i % 2]).wait()

    def mm_unit(w, a_ref, epilogue):
        l, kind = w
        ntiles = gath[kind].shape[2] // nt if kind != DOWN else 2 * (gath[kind].shape[2] // nu)

        def unit(i):
            tile_wait(i)

            @pl.when(i + 1 < ntiles)
            def _():
                tile_start(w, i + 1)

            if kind == DOWN:
                n, k = i // 2, i % 2
                n0 = pl.multiple_of(n * nu, 128)
                res = sum(
                    jnp.dot(a_ref[:, pl.ds(pl.multiple_of((2 * k + s) * kt, 128), kt)], wt[i % 2, :, s * nu:(s + 1) * nu],
                            preferred_element_type=F32) for s in range(2))
                epilogue(res, pl.ds(n0, nu), n0, k)
                return
            for s in range(nt // nu):
                n0 = pl.multiple_of(i * nt + s * nu, 128)
                res = jnp.dot(a_ref[...], wt[i % 2, :, s * nu:(s + 1) * nu], preferred_element_type=F32)
                epilogue(res, pl.ds(n0, nu), n0, 0)

        return ntiles, unit, lambda: tile_start(w, 0)

    def gelu_tanh(v):
        half = 0.5 * v
        return half + half * jnp.tanh(v * (GELU_C + (GELU_C * 0.044715) * (v * v)))

    def qkv_epi(l):
        def epi(res, nsl, n0, k):
            qkv[:, nsl] = (res + vec(l, B_QKV, n0, nu)).astype(BF16)

        return epi

    def out_epi(l):
        def epi(res, nsl, n0, k):
            x[:, nsl] = (x[:, nsl].astype(F32) + (res + vec(l, B_OUT, n0, nu))).astype(BF16)

        return epi

    def up_epi(l):
        def epi(res, nsl, n0, k):
            g[:, nsl] = gelu_tanh(res + vec(l, B_UP, n0, nu)).astype(BF16)

        return epi

    def down_epi(l):
        def epi(res, nsl, n0, k):
            @pl.when(k == 0)
            def _():
                acc[:, nsl] = res

            @pl.when(k == 1)
            def _():
                x[:, nsl] = (x[:, nsl].astype(F32) + (acc[:, nsl] + res + vec(l, B_DOWN, n0, nu))).astype(BF16)

        return epi

    seq = 2 * 128
    hg = 4

    def attn_unit():
        lane = lax.broadcasted_iota(jnp.int32, (1, seq), 1)
        gw = hg * hd
        scale = hd ** -0.5 * math.log2(math.e)

        def window(q2, k2, v2, offs):
            ms = [jnp.logical_and(lane >= o, lane < o + hd).astype(BF16) for o in offs]
            ks = jnp.concatenate([k2 * m for m in ms], axis=0)
            vs = jnp.concatenate([v2 * m for m in ms], axis=0)
            s = lax.dot_general(q2, ks, (((1,), (1,)), ((), ())), preferred_element_type=F32)
            ps = []
            for i in range(len(offs)):
                si = s[:, i * seq:(i + 1) * seq]
                e = jnp.exp2((si - jnp.max(si, axis=-1, keepdims=True)) * scale)
                ps.append((e * (1.0 / jnp.sum(e, axis=-1, keepdims=True))).astype(BF16))
            return jnp.dot(jnp.concatenate(ps, axis=1), vs, preferred_element_type=F32)

        def unit(u):
            img, grp = u // (heads // hg), u % (heads // hg)
            msl = pl.ds(pl.multiple_of(img * seq, seq), seq)

            def win_(base, off):
                return qkv[msl, pl.ds(pl.multiple_of(base * width + grp * gw + off, 128), seq)]

            o0 = window(win_(0, 0), win_(1, 0), win_(2, 0), (0, hd))
            o1 = window(win_(0, 128), win_(1, 128), win_(2, 128), (2 * hd - 128, 3 * hd - 128))
            c0 = grp * gw
            h[msl, pl.ds(pl.multiple_of(c0, 128), 128)] = o0[:, :128].astype(BF16)
            h[msl, pl.ds(pl.multiple_of(c0 + 128, 128), 128)] = (o0[:, 128:] + o1[:, :128]).astype(BF16)
            h[msl, pl.ds(pl.multiple_of(c0 + 256, 128), 128)] = o1[:, 128:].astype(BF16)

        return (rows // seq) * (heads // hg), unit

    def build_vectors():
        wait_bytes(vecg.at[pl.ds(0, nz)], vec_d)
        nd = nz * CORES
        for a in range(nd // 4):
            s = vecg[4 * a].astype(F32)
            for r in range(1, 4):
                s = s + vecg[4 * a + r].astype(F32)
            for l in range(2):
                for k in (LN1_S, LN1_B, B_OUT, LN2_S, LN2_B, B_DOWN):
                    wv = width // (nd // 4)
                    vrow[2 * k + l:2 * k + l + 1, a * wv:(a + 1) * wv] = s[2 * k + l:2 * k + l + 1, :wv]
                wv = width // (nd // 4)
                for seg in range(3):
                    row = l + (2 * B_QKV if seg == 0 else SEG_ROWS + 2 * seg)
                    at = (3 * a + seg) * wv
                    vrow[2 * B_QKV + l:2 * B_QKV + l + 1, at:at + wv] = s[row:row + 1, :wv]
        wv = vrow.shape[1] // nd
        for o in range(nd):
            s = vecg[o].astype(F32)
            for l in range(2):
                vrow[2 * B_UP + l:2 * B_UP + l + 1, o * wv:(o + 1) * wv] = s[2 * B_UP + l:2 * B_UP + l + 1, :wv]

    last = GROUPS[-1][-1]
    zrows = CORES * win[DOWN].shape[1]
    dq = width // 4

    def slot_copies(t):
        za, zb = (z - t + nz) % nz, (z + t) % nz
        for n, (zz, q, r0, c0) in enumerate(((za, 0, 0, 0), (za, 2, 0, dq), (zb, 1, zrows, 0), (zb, 3, zrows, dq))):
            yield pltpu.make_async_copy(
                gath[DOWN].at[last[0], pl.ds(pl.multiple_of(zz * zrows, 8), zrows), pl.ds(q * dq, dq)],
                wl.at[t % 2, pl.ds(r0, zrows), pl.ds(c0, dq)], tile_sem.at[t % 2])

    def slot_ready(t):
        l, kind = last
        wait_bytes(gath[kind].at[l, pl.ds(0, win[kind].shape[1]), :], rec_l.at[t])
        for cp in slot_copies(t):
            cp.start()

    def slot_wait(t):
        pltpu.make_async_copy(wl.at[t % 2], wl.at[t % 2], tile_sem.at[t % 2]).wait()

    def slot_compute(t):
        za, zb = (z - t + nz) % nz, (z + t) % nz

        for zz, r0, c0 in ((za, 0, 0), (zb, zrows, 2 * dq)):
            for nn in range(2 * dq // nu):
                csl = slice(c0 + nn * nu, c0 + (nn + 1) * nu)
                acc[:, csl] += jnp.dot(g[:, pl.ds(pl.multiple_of(zz * zrows, 128), zrows)],
                                       wl[t % 2, r0:r0 + zrows, nn * nu:(nn + 1) * nu], preferred_element_type=F32)

    vec_mine = vecg.at[f]
    load_x = pltpu.make_async_copy(x_in, x, out_sem.at[0])
    load_v = pltpu.make_async_copy(vec_in, vec_mine, out_sem.at[1])

    def own_load(kind):
        return pltpu.make_async_copy(win[kind], bounce[kind], loc.at[kind])

    def own_store(l, kind):
        r = shard_rows(kind)
        return pltpu.make_async_copy(bounce[kind].at[l], gath[kind].at[l, pl.ds(pl.multiple_of(f * r, 8), r), :], loc.at[4 * (l + 1) + kind])

    def load_raw(l):
        return pltpu.make_async_copy(win[QKV].at[l], raw, loc.at[QKV])

    def relayout(l, first, r):
        nh = raw.shape[1]
        wide, groups = r // 8, nh // hg

        def unit(u):
            @pl.when(u < wide)
            def _():
                raw32[pl.ds(pl.multiple_of(u * 8 * nh, 8), 8 * nh), :] = raw[pl.ds(pl.multiple_of(first + u * 8, 8), 8)].astype(F32).reshape(8 * nh, hd)

            @pl.when(u >= wide)
            def _():
                i = u - wide
                src = lax.broadcasted_iota(jnp.int32, (hd, hg * hd), 0)
                dst = lax.broadcasted_iota(jnp.int32, (hd, hg * hd), 1)
                res = sum(
                    jnp.dot(raw32[pl.ds(hg * i + k, r, stride=nh), :].astype(BF16), (dst == src + k * hd).astype(BF16),
                            preferred_element_type=F32) for k in range(hg))
                bounce[QKV][l, pl.ds(pl.multiple_of(first, 8), r), pl.ds(pl.multiple_of(i * hg * hd, 128), hg * hd)] = res.astype(BF16)

        return wide + groups, unit

    load_raw(0).start()
    load_x.start()
    for kind in (OUT, UP, DOWN):
        own_load(kind).start()
    barrier = pltpu.get_barrier_semaphore()
    for dev in (up_dev, dn_dev, sib_dev, x_dev, y_dev):
        pl.semaphore_signal(barrier, inc=1, device_id=dev, device_id_type=MESH)
    half_rows = raw.shape[0] // 2
    mine, other = par * half_rows, (1 - par) * half_rows

    def half_store(first):
        r = shard_rows(QKV)
        return pltpu.make_async_copy(bounce[QKV].at[0, pl.ds(pl.multiple_of(first, 8), half_rows)],
                                     gath[QKV].at[0, pl.ds(pl.multiple_of(f * r + first, 8), half_rows), :], loc.at[4 + QKV])

    def relay_half(first):
        n_re, re0 = relayout(0, first, half_rows)
        lax.fori_loop(0, n_re, lambda u, cc: (re0(u), cc)[1], 0)
        half_store(first).start()

    pl.semaphore_wait(barrier, 5)
    for j in range(SUB):
        own_send(0, j, (OUT,))
    own_send(1, 0)
    load_raw(0).wait()
    relay_half(mine)
    _pack(vin, vown)
    save_v = pltpu.make_async_copy(vown, vec_in, out_sem.at[1])
    save_v.start()
    half_store(mine).wait()
    for j in range(SUB):
        own_send(0, j, (QKV,))
    save_v.wait()
    remote(vec_in, vec_mine, snd_v.at[0], vec_a.at[0], up_dev).start()
    remote(vec_in, vec_mine, snd_v.at[1], vec_b.at[0], dn_dev).start()
    load_v.start()
    relay_half(other)
    load_raw(1).start()
    half_store(other).wait()
    remote(vec_in, vec_mine, snd_v.at[2], vec_d, sib_dev).start()
    own_d2d(0)
    for kind in (OUT, UP, DOWN):
        own_load(kind).wait()
        for l in range(2):
            own_store(l, kind).start()

    def start_group(grp, first=(), second=()):
        run(grp, 0, SUB, *first)
        run(grp, SUB, SUB + 1, *second)
        await_group(grp - 1)
        own_d2d(grp)

    qkv0_n, qkv0_u, qkv0_s = mm_unit((0, QKV), h, qkv_epi(0))
    out0_n, out0_u, out0_s = mm_unit((0, OUT), h, out_epi(0))
    up0_n, up0_u, up0_s = mm_unit((0, UP), h, up_epi(0))
    down0_n, down0_u, down0_s = mm_unit((0, DOWN), g, down_epi(0))
    qkv1_n, qkv1_u, qkv1_s = mm_unit((1, QKV), h, qkv_epi(1))
    out1_n, out1_u, out1_s = mm_unit((1, OUT), h, out_epi(1))
    up1_n, up1_u, up1_s = mm_unit((1, UP), h, up_epi(1))
    at_n, at_u = attn_unit()

    def begin(s):
        if COMPUTE:
            s()

    run(0, 0, SUB)
    load_raw(1).wait()
    run(0, SUB, 13, *relayout(1, 0, raw.shape[0]))
    own_store(1, QKV).start()
    run(0, 13, 14)
    load_v.wait()
    load_x.wait()
    for kind in range(4):
        for l in range(2):
            if (l, kind) != (0, QKV):
                own_store(l, kind).wait()
    build_vectors()
    run(0, 14, ticks, *ln_unit(0, LN1_S, LN1_B))

    start_group(1)
    begin(qkv0_s)
    run(1, 4, 13, qkv0_n, qkv0_u)
    run(1, 13, ticks, at_n, at_u)

    begin(out0_s)
    start_group(2, (2, out0_u), (out0_n - 2, lambda u: out0_u(u + 2)))
    begin(up0_s)
    run(2, 4, 7, *ln_unit(0, LN2_S, LN2_B))
    run(2, 7, ticks, up0_n, up0_u)

    start_group(3)
    begin(down0_s)
    run(3, 4, 17, down0_n, down0_u)
    run(3, 17, ticks, *ln_unit(1, LN1_S, LN1_B))
    acc[...] = jnp.zeros_like(acc)

    start_group(4)
    begin(qkv1_s)
    run(4, 4, 11, qkv1_n, qkv1_u)
    run(4, 11, 17, at_n, at_u)
    begin(out1_s)
    run(4, 17, ticks, out1_n, out1_u)

    start_group(5, ln_unit(1, LN2_S, LN2_B))
    begin(up1_s)
    run(5, 4, 15, up1_n, up1_u)
    slot_ready(0)

    def slots(u):
        slot_wait(u)
        slot_ready(u + 1)
        slot_compute(u)

    if not COMPUTE:
        slot_wait(0)
    run(5, 15, ticks, steps - 1, slots)
    if COMPUTE:
        for j in range(SUB):
            xy_arrive(5, steps, j)
            if j == 0:
                slot_wait(steps - 1)
                slot_compute(steps - 1)
        slot_ready(steps)
        slot_wait(steps)
        slot_compute(steps)
    else:
        for j in range(SUB):
            xy_arrive(5, steps, j)
        for t in range(1, steps + 1):
            slot_ready(t)
            slot_wait(t)
    for mb in range(mblocks):
        msl = pl.ds(mb * mrows, mrows)
        for n, q in enumerate((0, 2, 1, 3)):
            csl = slice(q * dq, (q + 1) * dq)
            x[msl, csl] = (x[msl, csl].astype(F32) + (acc[msl, n * dq:(n + 1) * dq] + vec(1, B_DOWN, q * dq, dq))).astype(BF16)
        pltpu.make_async_copy(x.at[msl], out_ref.at[msl], out_sem.at[mb]).start()
    for w in [w for grp in GROUPS for w in grp]:
        for sem in (snd_a, snd_b, snd_x, snd_y):
            wait_bytes(amount(w, steps), sem.at[wid(w)])
        wait_bytes(amount(w, 4 * nz), snd_d.at[wid(w)])
    wait_bytes(vecg.at[pl.ds(0, nz // 2)], snd_v.at[0])
    wait_bytes(vecg.at[pl.ds(0, nz // 2 - 1)], snd_v.at[1])
    wait_bytes(vecg.at[pl.ds(0, nz)], snd_v.at[2])
    for mb in range(mblocks):
        msl = pl.ds(mb * mrows, mrows)
        pltpu.make_async_copy(x.at[msl], out_ref.at[msl], out_sem.at[mb]).wait()


def _copy(src, dst, buf, sem_in, sem_out):
    n = buf.shape[0] // COPIES
    ins = [pltpu.make_async_copy(src.at[pl.ds(i * n, n)], buf.at[pl.ds(i * n, n)], sem_in.at[i]) for i in range(COPIES)]
    outs = [pltpu.make_async_copy(buf.at[pl.ds(i * n, n)], dst.at[pl.ds(i * n, n)], sem_out.at[i]) for i in range(COPIES)]
    for cp in ins:
        cp.start()
    for cp, out in zip(ins, outs):
        cp.wait()
        out.start()
    for out in outs:
        out.wait()


def solution(mesh):
    batch_spec = P(('dp', 'fsdp'), None, None)
    vector_spec = P(None, 'fsdp')
    matrix_spec = P(None, 'fsdp', None)
    in_specs = (batch_spec, vector_spec, vector_spec, P(None, 'fsdp', None, None, None), vector_spec, matrix_spec, vector_spec,
                vector_spec, vector_spec, matrix_spec, vector_spec, matrix_spec, vector_spec)
    nd = mesh.shape['fsdp']
    nz = nd // CORES
    ny = math.isqrt(mesh.shape['dp'])

    def local(images, ln1_s, ln1_b, w_qkv, b_qkv, w_out, b_out, ln2_s, ln2_b, w_up, b_up, w_down, b_down):
        nimg, seq, width = images.shape
        layers = w_qkv.shape[0]
        heads, hd = w_qkv.shape[3], w_qkv.shape[4]
        rows = nimg * seq
        x = images.reshape(rows, width)
        vw = 4 * b_out.shape[1]
        vr = -(-(layers * 10) // 16) * 16
        vecs = (ln1_s, ln1_b, b_qkv, b_out, ln2_s, ln2_b, b_up, b_down)
        mats = (w_qkv.reshape(layers, w_qkv.shape[1], 3 * heads, hd), w_out, w_up, w_down)
        cols = (3 * width, width, w_up.shape[2], width)
        any_spec = pl.BlockSpec(memory_space=pl.ANY)
        dma = pltpu.SemaphoreType.DMA
        nw = 4 * layers
        gshapes = [jax.ShapeDtypeStruct((layers, nd * m.shape[1], n), BF16) for m, n in zip(mats, cols)]
        outs = pl.pallas_call(
            functools.partial(_kernel, (ny, nz, heads, hd)),
            out_shape=[jax.ShapeDtypeStruct((rows, width), BF16), jax.ShapeDtypeStruct((vr, vw), BF16)] + gshapes,
            in_specs=[any_spec] + [pl.BlockSpec(memory_space=pltpu.VMEM)] * 8 + [any_spec] * 4,
            out_specs=[any_spec] * 6,
            scratch_shapes=[
                pltpu.VMEM((rows, width), BF16),
                pltpu.VMEM((rows, width), BF16),
                pltpu.VMEM((rows, 3 * width), BF16),
                pltpu.VMEM((rows, w_up.shape[2]), BF16),
                pltpu.VMEM((rows, width), F32),
                pltpu.VMEM((2, width, width // 3), BF16),
                pltpu.VMEM((2, width, width // 2), BF16),
                *[pltpu.VMEM((*m.shape[:2], n), BF16) for m, n in zip(mats, cols)],
                pltpu.VMEM((nd, vr, vw), BF16),
                pltpu.VMEM((layers * 8, w_up.shape[2]), F32),
                pltpu.VMEM((vr, vw), BF16),
                pltpu.VMEM(mats[0].shape[1:], BF16),
                pltpu.VMEM((mats[0].shape[1] * 3 * heads, hd), F32),
                *[dma((nw, nz - 1, SUB))] * 4,
                dma((nw,)),
                dma((nz,)),
                *[dma((nw,))] * 5,
                dma((3,)),
                dma((nz // 2,)),
                dma((nz // 2,)),
                dma,
                dma((4 * (layers + 1),)),
                dma((2,)),
                dma((3,)),
            ],
            compiler_params=pltpu.CompilerParams(collective_id=0, has_side_effects=True, vmem_limit_bytes=56 * 1024 * 1024),
        )(x, *vecs, *mats)
        out = pl.pallas_call(
            _copy,
            out_shape=jax.ShapeDtypeStruct((rows, width), BF16),
            in_specs=[any_spec],
            out_specs=any_spec,
            scratch_shapes=[pltpu.VMEM((rows, width), BF16), dma((COPIES,)), dma((COPIES,))],
        )(outs[0])
        return out.reshape(nimg, seq, width)

    return jax.shard_map(local, mesh=mesh, in_specs=in_specs, out_specs=batch_spec, check_vma=False)
```
